8 devices in a mesh: rep: 1 (over z), data: 8 (over y, x, core).
Axes of the slice: x: 2, y: 2, z: 1, core: 2. Of those that a mesh axis runs over, the one named last changes fastest.
Arguments:
- hidden: bfloat16 [8192, 5120], P(('rep', 'data'))
- adapter_id: int32 [8192], P(('rep', 'data'))
- w_gate: bfloat16 [5120, 13824], replicated
- w_up: bfloat16 [5120, 13824], replicated
- w_down: bfloat16 [13824, 5120], replicated
- a_gate: bfloat16 [256, 5120, 8], replicated
- b_gate: bfloat16 [256, 8, 13824], P('data')
- a_up: bfloat16 [256, 5120, 8], replicated
- b_up: bfloat16 [256, 8, 13824], P('data')
- a_down: bfloat16 [256, 13824, 8], replicated
- b_down: bfloat16 [256, 8, 5120], P('data')
Outputs:
- output: bfloat16 [8192, 5120], P(('rep', 'data'))
All inputs are finite; a program needn't handle non-finite values.
Results may differ from the reference program's by a relative error of at most 0.00726582.
Values are sent between devices in bfloat16 or wider.
A program may use at most 2.25 GiB of HBM per device.

```python
import jax
import jax.numpy as jnp
from jax import lax

D = 5120
FF = 13824
RANK = 8
ADAPTERS = 256
GROUP = 8
TOKENS_DEV = 1024
TOKENS = 8192
CAP = 512
PER_OWNER = ADAPTERS // GROUP
ROW_BLOCK = min(64, TOKENS)
LORA_SCALE = 2.0


def draw_ids(key):
    key_hot, key_src, key_one, key_two = jax.random.split(key, 4)
    hot_owner = jax.random.randint(key_hot, (), 0, GROUP)

    def one_source(src_key):
        key_slot, key_order = jax.random.split(src_key)
        slot_order = jax.random.permutation(key_slot, (GROUP - 1) * (CAP - 1))
        extra_rank = slot_order[:TOKENS_DEV - CAP - GROUP + 1] // (CAP - 1)
        other_rank = jnp.concatenate([jnp.arange(GROUP - 1, dtype=jnp.int32), extra_rank.astype(jnp.int32)])
        other_owner = other_rank + (other_rank >= hot_owner).astype(jnp.int32)
        owner_ids = jnp.concatenate([jnp.full((CAP,), hot_owner, jnp.int32), other_owner])
        return jax.random.permutation(key_order, owner_ids)

    owner_ids = jax.vmap(one_source)(jax.random.split(key_src, GROUP)).reshape(TOKENS)
    pick_one = jax.random.randint(key_one, (TOKENS,), 0, PER_OWNER)
    pick_two = jax.random.randint(key_two, (TOKENS,), 0, PER_OWNER)
    return (owner_ids * PER_OWNER + jnp.minimum(pick_one, pick_two)).astype(jnp.int32)


def weight(key, shape, scale):
    return (jax.random.normal(key, shape, jnp.float32) * scale).astype(jnp.bfloat16)


def setup_inputs(seed: int = 0, part: int = 0) -> dict:
    base_key = jax.random.key(seed)
    part_key = jax.random.fold_in(base_key, part)
    key_rows, key_ids = jax.random.split(part_key)
    keys = jax.random.split(base_key, 9)
    return {
        'hidden': jax.random.normal(key_rows, (TOKENS, D), jnp.float32).astype(jnp.bfloat16),
        'adapter_id': draw_ids(key_ids),
        'w_gate': weight(keys[0], (D, FF), D ** -0.5),
        'w_up': weight(keys[1], (D, FF), D ** -0.5),
        'w_down': weight(keys[2], (FF, D), FF ** -0.5),
        'a_gate': weight(keys[3], (ADAPTERS, D, RANK), D ** -0.5),
        'b_gate': weight(keys[4], (ADAPTERS, RANK, FF), 0.15 * RANK ** -0.5),
        'a_up': weight(keys[5], (ADAPTERS, D, RANK), D ** -0.5),
        'b_up': weight(keys[6], (ADAPTERS, RANK, FF), 0.15 * RANK ** -0.5),
        'a_down': weight(keys[7], (ADAPTERS, FF, RANK), FF ** -0.5),
        'b_down': weight(keys[8], (ADAPTERS, RANK, D), 0.25 * RANK ** -0.5),
    }


def lora_delta(act_rows, a_rows, b_rows):
    low_rows = jnp.einsum('tk,tkr->tr', act_rows.astype(jnp.float32), a_rows.astype(jnp.float32)).astype(jnp.bfloat16)
    full_rows = jnp.einsum('tr,trm->tm', low_rows.astype(jnp.float32), b_rows.astype(jnp.float32))
    return (LORA_SCALE * full_rows).astype(jnp.bfloat16)


def reference(hidden, adapter_id, w_gate, w_up, w_down, a_gate, b_gate, a_up, b_up, a_down, b_down):
    def one_block(block):
        block_rows, block_ids = block
        gate_act = jnp.dot(block_rows, w_gate, preferred_element_type=jnp.float32) + lora_delta(block_rows, a_gate[block_ids], b_gate[block_ids]).astype(jnp.float32)
        up_act = jnp.dot(block_rows, w_up, preferred_element_type=jnp.float32) + lora_delta(block_rows, a_up[block_ids], b_up[block_ids]).astype(jnp.float32)
        hid_act = (jax.nn.silu(gate_act) * up_act).astype(jnp.bfloat16)
        down_act = jnp.dot(hid_act, w_down, preferred_element_type=jnp.float32) + lora_delta(hid_act, a_down[block_ids], b_down[block_ids]).astype(jnp.float32)
        return (block_rows.astype(jnp.float32) + down_act).astype(jnp.bfloat16)

    out_blocks = lax.map(one_block, (hidden.reshape(TOKENS // ROW_BLOCK, ROW_BLOCK, D), adapter_id.reshape(TOKENS // ROW_BLOCK, ROW_BLOCK)))
    return out_blocks.reshape(TOKENS, D)
```

```python
import jax
import jax.numpy as jnp
from jax import lax
from jax.experimental import pallas as pl
from jax.experimental.pallas import tpu as pltpu
from jax.sharding import PartitionSpec as P

SCALE = 2.0
HOT = 512
BLK = 112
COLD = 7
TF = 512
TD = 512
TK = 512
CHUNKS = (5, 8, 8, 6)
BF = jnp.bfloat16
F32 = jnp.float32
NT = (((1,), (1,)), ((), ()))
VMEM_LIMIT = 62 * 2**20


def mm(a, b):
    return jnp.dot(a, b, preferred_element_type=F32)


def mm_nt(a, b):
    return lax.dot_general(a, b, NT, preferred_element_type=F32)


def scaled(low, b):
    return (SCALE * mm(low, b)).astype(BF)


class Slots:
    def __init__(self, meta, rows):
        self.meta, self.last = meta, rows - BLK
        self.hot = meta[0]

    def owner(self, j):
        return self.meta[8 + j]

    def first(self, j):
        base = (self.meta[16 + j] // 16) * 16
        return pl.multiple_of(jnp.minimum(base, self.last), 16)

    def mask(self, j):
        start, end = self.meta[16 + j], self.meta[24 + j]
        return self._mask(self.first(j), start, jnp.minimum(end, (start // 16) * 16 + BLK))

    def _mask(self, first, low, high):
        row = first + lax.broadcasted_iota(jnp.int32, (BLK, 1), 0)
        return (row >= low) & (row < high)

    def extras(self, visit):
        @pl.when(self.meta[1] > 0)
        def _():
            def slot(j, carry):
                end = self.meta[24 + j]
                base = (self.meta[16 + j] // 16) * 16

                def more(b, carry):
                    low = base + b * BLK
                    first = pl.multiple_of(jnp.minimum(low, self.last), 16)
                    mask = self._mask(first, low, jnp.minimum(end, low + BLK))
                    visit(self.owner(j), pl.ds(first, BLK), mask)
                    return carry

                return lax.fori_loop(1, (end - base + BLK - 1) // BLK, more, carry)

            lax.fori_loop(0, COLD, slot, 0)


def sort_kernel(meta, rank_ref, loc_ref, x_ref, ag_ref, au_ref, xs_ref, lg_ref, lu_ref, pg_ref, pu_ref, perm, acc_g, acc_u, pad_g, pad_u):
    step = pl.program_id(0)
    s = Slots(meta, xs_ref.shape[0])

    @pl.when(step == 0)
    def _():
        row = lax.broadcasted_iota(jnp.int32, perm.shape, 0)
        perm[...] = jnp.where(row == rank_ref[...], 1.0, 0.0).astype(BF)
        for ref in (acc_g, acc_u, pad_g, pad_u):
            ref[...] = jnp.zeros_like(ref)

    xs_ref[...] = mm(perm[...], x_ref[...]).astype(BF)
    acc_g[:HOT] += mm_nt(xs_ref[:HOT, :], ag_ref[s.hot])
    acc_u[:HOT] += mm_nt(xs_ref[:HOT, :], au_ref[s.hot])
    for j in range(COLD):
        part = xs_ref[pl.ds(s.first(j), BLK), :]
        pad_g[j] += mm_nt(part, ag_ref[s.owner(j)])
        pad_u[j] += mm_nt(part, au_ref[s.owner(j)])

    def visit(owner, rs, mask):
        part = xs_ref[rs, :]
        acc_g[rs, :] += jnp.where(mask, mm_nt(part, ag_ref[owner]), 0.0)
        acc_u[rs, :] += jnp.where(mask, mm_nt(part, au_ref[owner]), 0.0)

    s.extras(visit)

    @pl.when(step == pl.num_programs(0) - 1)
    def _():
        own = (lax.broadcasted_iota(jnp.int32, acc_g.shape, 1) // 8) == loc_ref[...]
        lg_ref[...] = jnp.where(own, acc_g[...], 0.0).astype(BF)
        lu_ref[...] = jnp.where(own, acc_u[...], 0.0).astype(BF)
        col = lax.broadcasted_iota(jnp.int32, (BLK, 256), 1) // 8
        for j in range(COLD):
            keep = (col == loc_ref[pl.ds(s.first(j), BLK), :]) & s.mask(j)
            pg_ref[j] = jnp.where(keep, pad_g[j], 0.0).astype(BF)
            pu_ref[j] = jnp.where(keep, pad_u[j], 0.0).astype(BF)


def up_kernel(meta, x_ref, wg_ref, wu_ref, lg_ref, lu_ref, pg_ref, pu_ref, ad_ref, b_ref, hot_in, pad_in, rare_in,
              h_ref, hot_ref, pad_ref, rare_ref, g, u, dg, du):
    s = Slots(meta, x_ref.shape[0])

    @pl.when(pl.program_id(0) == 0)
    def _():
        hot_ref[...] = hot_in[...]
        pad_ref[...] = pad_in[...]
        rare_ref[...] = rare_in[...]

    for j in range(COLD):
        dg[j] = scaled(pg_ref[j], b_ref[s.owner(j), 0])
        du[j] = scaled(pu_ref[j], b_ref[s.owner(j), 1])
    g[...] = mm(x_ref[...], wg_ref[...])
    u[...] = mm(x_ref[...], wu_ref[...])
    g[:HOT] += scaled(lg_ref[:HOT, :], b_ref[s.hot, 0]).astype(F32)
    u[:HOT] += scaled(lu_ref[:HOT, :], b_ref[s.hot, 1]).astype(F32)
    for j in range(COLD):
        rs = pl.ds(s.first(j), BLK)
        g[rs, :] += dg[j].astype(F32)
        u[rs, :] += du[j].astype(F32)

    def visit(owner, rs, mask):
        g[rs, :] += scaled(jnp.where(mask, lg_ref[rs, :].astype(F32), 0.0).astype(BF), b_ref[owner, 0]).astype(F32)
        u[rs, :] += scaled(jnp.where(mask, lu_ref[rs, :].astype(F32), 0.0).astype(BF), b_ref[owner, 1]).astype(F32)

    s.extras(visit)
    h_ref[...] = (jax.nn.silu(g[...]) * u[...]).astype(BF)
    hot_ref[...] += mm_nt(h_ref[:HOT, :], ad_ref[s.hot])
    for j in range(COLD):
        pad_ref[j] += mm_nt(h_ref[pl.ds(s.first(j), BLK), :], ad_ref[s.owner(j)])

    def visit_d(owner, rs, mask):
        rare_ref[rs, :] += jnp.where(mask, mm_nt(h_ref[rs, :], ad_ref[owner]), 0.0)

    s.extras(visit_d)


def part_kernel(h_ref, w_ref, *rest):
    y_ref = rest[-1]
    acc = mm(h_ref[...], w_ref[...])
    y_ref[...] = acc if len(rest) == 1 else acc + rest[0][...]


def down_kernel(meta, rank_ref, loc_ref, hot_ref, pad_ref, rare_ref, xs_ref, h_ref, w_ref, yin_ref, b_ref, o_ref, perm, low, pad, y, dy):
    s = Slots(meta, xs_ref.shape[0])

    @pl.when(pl.program_id(0) == 0)
    def _():
        col = lax.broadcasted_iota(jnp.int32, perm.shape, 1)
        perm[...] = jnp.where(col == rank_ref[...], 1.0, 0.0).astype(BF)
        total = rare_ref
        own = (lax.broadcasted_iota(jnp.int32, total.shape, 1) // 8) == loc_ref[...]
        low[...] = jnp.where(own, total[...], 0.0).astype(BF)
        low[:HOT] = jnp.where(own[:HOT], hot_ref[...], 0.0).astype(BF)
        col = lax.broadcasted_iota(jnp.int32, (BLK, 256), 1) // 8
        for j in range(COLD):
            keep = (col == loc_ref[pl.ds(s.first(j), BLK), :]) & s.mask(j)
            pad[j] = jnp.where(keep, pad_ref[j], 0.0).astype(BF)

    for j in range(COLD):
        dy[j] = scaled(pad[j], b_ref[s.owner(j)])
    y[...] = mm(h_ref[...], w_ref[...]) + yin_ref[...]
    y[:HOT] += scaled(low[:HOT, :], b_ref[s.hot]).astype(F32)
    for j in range(COLD):
        y[pl.ds(s.first(j), BLK), :] += dy[j].astype(F32)

    def visit(owner, rs, mask):
        y[rs, :] += scaled(jnp.where(mask, low[rs, :].astype(F32), 0.0).astype(BF), b_ref[owner]).astype(F32)

    s.extras(visit)
    done = (xs_ref[...].astype(F32) + y[...]).astype(BF)
    o_ref[...] = mm(perm[...], done).astype(BF)


def params(limit=VMEM_LIMIT):
    return pltpu.CompilerParams(vmem_limit_bytes=limit, dimension_semantics=('arbitrary',))


def const(shape):
    return pl.BlockSpec(shape, lambda i, *_: (0,) * len(shape), pipeline_mode=pl.Buffered(1))


def cols(shape, off=0):
    lead = (0,) * (len(shape) - 1)
    return pl.BlockSpec(shape, lambda i, *_: lead + (i + off,))


def row_part(rows, width, off):
    return pl.BlockSpec((pl.Element(rows), pl.Element(width)), lambda i, *_: (off, i * width))


def shape(dims, dtype):
    return jax.ShapeDtypeStruct(dims, dtype)


def cost(flops, nbytes, trans=0):
    return pl.CostEstimate(flops=int(flops), bytes_accessed=int(nbytes), transcendentals=trans)


def sort_call(meta, rank_row, loc_col, hidden, ag, au):
    rows, d = hidden.shape
    low, pad = (rows, 256), (COLD, BLK, 256)
    return pl.pallas_call(
        sort_kernel,
        grid_spec=pltpu.PrefetchScalarGridSpec(
            num_scalar_prefetch=1, grid=(d // TK,),
            in_specs=[const((1, rows)), const((rows, 1)), cols((rows, TK)), cols((8, 256, TK)), cols((8, 256, TK))],
            out_specs=[cols((rows, TK)), const(low), const(low), const(pad), const(pad)],
            scratch_shapes=[pltpu.VMEM((rows, rows), BF), pltpu.VMEM(low, F32), pltpu.VMEM(low, F32), pltpu.VMEM(pad, F32), pltpu.VMEM(pad, F32)]),
        out_shape=[shape((rows, d), BF), shape(low, BF), shape(low, BF), shape(pad, BF), shape(pad, BF)],
        compiler_params=params(40 * 2**20),
        cost_estimate=cost(2 * rows * d * (rows + 700), 4 * rows * d + 8192 * d),
        name='sort_rows',
    )(meta, rank_row, loc_col, hidden, ag, au)


def up_call(meta, xs, wg, wu, lows, ad, b, acc, off, width):
    rows, d = xs.shape
    f = width * TF
    low, pad = (rows, 256), (COLD, BLK, 256)
    accs = [const((HOT, 256)), const(pad), const(low)]
    return pl.pallas_call(
        up_kernel,
        grid_spec=pltpu.PrefetchScalarGridSpec(
            num_scalar_prefetch=1, grid=(width,),
            in_specs=[const((rows, d)), cols((d, TF), off), cols((d, TF), off), const(low), const(low), const(pad), const(pad),
                      cols((8, 256, TF), off), cols((8, 2, 256, TF))] + accs,
            out_specs=[cols((rows, TF))] + accs,
            scratch_shapes=[pltpu.VMEM((rows, TF), F32), pltpu.VMEM((rows, TF), F32), pltpu.VMEM((COLD, BLK, TF), BF), pltpu.VMEM((COLD, BLK, TF), BF)]),
        out_shape=[shape((rows, f), BF), shape((HOT, 256), F32), shape(pad, F32), shape(low, F32)],
        compiler_params=params(),
        cost_estimate=cost(4 * rows * d * f * 1.2, 4 * d * f + 2 * rows * (d + f) + 12288 * f, rows * f),
        name='gate_up',
    )(meta, xs, wg, wu, *lows, ad, b, *acc)


def part_call(h, w, y, off):
    rows, f = h.shape
    d = w.shape[1]
    extra = [] if y is None else [y]
    return pl.pallas_call(
        part_kernel,
        grid=(d // TD,),
        in_specs=[const(h.shape), row_part(f, TD, off * TF)] + [cols((rows, TD))] * len(extra),
        out_specs=cols((rows, TD)),
        out_shape=shape((rows, d), F32),
        input_output_aliases={2: 0} if extra else {},
        compiler_params=params(40 * 2**20),
        cost_estimate=cost(2 * rows * d * f, 2 * d * f + 2 * rows * f + 8 * rows * d),
        name='down_part',
    )(h, w, *extra)


def down_call(meta, rank_col, loc_col, acc, xs, h, w, y, b, off):
    rows, d = xs.shape
    f = h.shape[1]
    low, pad = (rows, 256), (COLD, BLK, 256)
    return pl.pallas_call(
        down_kernel,
        grid_spec=pltpu.PrefetchScalarGridSpec(
            num_scalar_prefetch=1, grid=(d // TD,),
            in_specs=[const((rows, 1)), const((rows, 1)), const((HOT, 256)), const(pad), const(low), cols((rows, TD)),
                      const(h.shape), row_part(f, TD, off * TF), cols((rows, TD)), cols((8, 256, TD))],
            out_specs=cols((rows, TD)),
            scratch_shapes=[pltpu.VMEM((rows, rows), BF), pltpu.VMEM(low, BF), pltpu.VMEM(pad, BF), pltpu.VMEM((rows, TD), F32), pltpu.VMEM((COLD, BLK, TD), BF)]),
        out_shape=shape((rows, d), BF),
        compiler_params=params(),
        cost_estimate=cost(2 * rows * d * (f + rows + 512), 2 * (d * f + rows * f + 2 * rows * d + 2048 * d) + 4 * rows * d),
        name='down',
    )(meta, rank_col, loc_col, *acc, xs, h, w, y, b)


def gather(own):
    return lax.all_gather(own, 'data', axis=0, tiled=False)


def solution(mesh):
    row_spec = P(('rep', 'data'), None)
    tok_spec = P(('rep', 'data'))
    full_two = P(None, None)
    full_three = P(None, None, None)
    owned = P('data', None, None)

    def device_fn(hidden, adapter_id, w_gate, w_up, w_down, a_gate, b_gate, a_up, b_up, a_down, b_down):
        rows, d = hidden.shape
        f = w_gate.shape[1]
        bg, bu, bd = b_gate.reshape(256, f), b_up.reshape(256, f), b_down.reshape(256, d)
        ag, au, ad = (jnp.swapaxes(a, 1, 2).reshape(8, 256, a.shape[1]) for a in (a_gate, a_up, a_down))

        packs, offs, off = [], [], 0
        for width in CHUNKS:
            cut = slice(off * TF, (off + width) * TF)
            packs.append(gather(jnp.stack([bg[:, cut], bu[:, cut]])))
            offs.append(off)
            off += width
        b_all = gather(bd)

        owner = adapter_id // 32
        owners = jnp.arange(8, dtype=jnp.int32)
        token = jnp.arange(rows, dtype=jnp.int32)
        count = jnp.sum((owner[:, None] == owners[None, :]).astype(jnp.int32), axis=0)
        hot = jnp.argmax(count).astype(jnp.int32)
        key = jnp.where(owner == hot, -1, owner)
        before = (key[None, :] < key[:, None]) | ((key[None, :] == key[:, None]) & (token[None, :] < token[:, None]))
        rank = jnp.sum(before.astype(jnp.int32), axis=1)
        loc = jnp.sum(jnp.where(rank[None, :] == token[:, None], (adapter_id % 32)[None, :], 0), axis=1)
        cold = jnp.arange(COLD, dtype=jnp.int32)
        cold = cold + (cold >= hot).astype(jnp.int32)
        start = HOT + jnp.sum(jnp.where((owners[None, :] < cold[:, None]) & (owners[None, :] != hot), count[None, :], 0), axis=1)
        end = start + jnp.sum(jnp.where(owners[None, :] == cold[:, None], count[None, :], 0), axis=1)
        extra = jnp.any(end - (start // 16) * 16 > BLK).astype(jnp.int32)
        zero = jnp.zeros((1,), jnp.int32)
        meta = jnp.concatenate([jnp.stack([hot, extra]), jnp.zeros((6,), jnp.int32), cold, zero, start, zero, end, zero]).astype(jnp.int32)

        xs, *lows = sort_call(meta, rank[None, :], loc[:, None], hidden, ag, au)
        acc = [jnp.zeros((HOT, 256), F32), jnp.zeros((COLD, BLK, 256), F32), jnp.zeros((rows, 256), F32)]
        y = None
        for i, (pack, first, width) in enumerate(zip(packs, offs, CHUNKS)):
            h, *acc = up_call(meta, xs, w_gate, w_up, lows, ad, pack, acc, first, width)
            if i < len(CHUNKS) - 1:
                y = part_call(h, w_down, y, first)
        return down_call(meta, rank[:, None], loc[:, None], acc, xs, h, w_down, y, b_all, offs[-1])

    return jax.shard_map(device_fn, mesh=mesh, in_specs=(row_spec, tok_spec, full_two, full_two, full_two, full_three, owned, full_three, owned, full_three, owned), out_specs=row_spec, check_vma=False)
```

```python
import functools

import jax
import jax.numpy as jnp
from jax import lax
from jax.experimental import pallas as pl
from jax.experimental.pallas import tpu as pltpu
from jax.sharding import PartitionSpec as P

SCALE = 2.0
HOT = 512
BLK = 112
COLD = 7
TF = 512
TD = 512
TK = 1024
CHUNKS = (8, 9, 10)
BF = jnp.bfloat16
F32 = jnp.float32
NT = (((1,), (1,)), ((), ()))
VMEM_LIMIT = 50 * 2**20
UP_LIMIT = 60 * 2**20
WHOLE = pl.BlockSpec(memory_space=pltpu.VMEM)


def mm(a, b):
    return jnp.dot(a, b, preferred_element_type=F32)


def mm_nt(a, b):
    return lax.dot_general(a, b, NT, preferred_element_type=F32)


def scaled(low, b):
    return (SCALE * mm(low, b)).astype(BF)


class Slots:
    def __init__(self, meta, rows):
        self.meta, self.last = meta, rows - BLK
        self.hot = meta[0]

    def owner(self, j):
        return self.meta[8 + j]

    def first(self, j):
        base = (self.meta[16 + j] // 16) * 16
        return pl.multiple_of(jnp.minimum(base, self.last), 16)

    def mask(self, j):
        start, end = self.meta[16 + j], self.meta[24 + j]
        return self._mask(self.first(j), start, jnp.minimum(end, (start // 16) * 16 + BLK))

    def _mask(self, first, low, high):
        row = first + lax.broadcasted_iota(jnp.int32, (BLK, 1), 0)
        return (row >= low) & (row < high)

    def extras(self, visit):
        @pl.when(self.meta[1] > 0)
        def _():
            def slot(j, carry):
                end = self.meta[24 + j]
                base = (self.meta[16 + j] // 16) * 16

                def more(b, carry):
                    low = base + b * BLK
                    first = pl.multiple_of(jnp.minimum(low, self.last), 16)
                    mask = self._mask(first, low, jnp.minimum(end, low + BLK))
                    visit(self.owner(j), pl.ds(first, BLK), mask)
                    return carry

                return lax.fori_loop(1, (end - base + BLK - 1) // BLK, more, carry)

            lax.fori_loop(0, COLD, slot, 0)


def sort_kernel(meta, rank_ref, loc_ref, x_ref, ag_ref, au_ref, xs_ref, lg_ref, lu_ref, pg_ref, pu_ref, perm, acc_g, acc_u, pad_g, pad_u):
    step = pl.program_id(0)
    s = Slots(meta, xs_ref.shape[0])

    @pl.when(step == 0)
    def _():
        row = lax.broadcasted_iota(jnp.int32, perm.shape, 0)
        perm[...] = jnp.where(row == rank_ref[...], 1.0, 0.0).astype(BF)
        for ref in (acc_g, acc_u, pad_g, pad_u):
            ref[...] = jnp.zeros_like(ref)

    xs_ref[...] = mm(perm[...], x_ref[...]).astype(BF)
    acc_g[:HOT] += mm_nt(xs_ref[:HOT, :], ag_ref[s.hot])
    acc_u[:HOT] += mm_nt(xs_ref[:HOT, :], au_ref[s.hot])
    for j in range(COLD):
        part = xs_ref[pl.ds(s.first(j), BLK), :]
        pad_g[j] += mm_nt(part, ag_ref[s.owner(j)])
        pad_u[j] += mm_nt(part, au_ref[s.owner(j)])

    def visit(owner, rs, mask):
        part = xs_ref[rs, :]
        acc_g[rs, :] += jnp.where(mask, mm_nt(part, ag_ref[owner]), 0.0)
        acc_u[rs, :] += jnp.where(mask, mm_nt(part, au_ref[owner]), 0.0)

    s.extras(visit)

    @pl.when(step == pl.num_programs(0) - 1)
    def _():
        own = (lax.broadcasted_iota(jnp.int32, acc_g.shape, 1) // 8) == loc_ref[...]
        lg_ref[...] = jnp.where(own, acc_g[...], 0.0).astype(BF)
        lu_ref[...] = jnp.where(own, acc_u[...], 0.0).astype(BF)
        col = lax.broadcasted_iota(jnp.int32, (BLK, 256), 1) // 8
        for j in range(COLD):
            keep = (col == loc_ref[pl.ds(s.first(j), BLK), :]) & s.mask(j)
            pg_ref[j] = jnp.where(keep, pad_g[j], 0.0).astype(BF)
            pu_ref[j] = jnp.where(keep, pad_u[j], 0.0).astype(BF)


def pack_kernel(g_ref, u_ref, o_ref):
    o_ref[0] = g_ref[...]
    o_ref[1] = u_ref[...]


def base_kernel(x_ref, wg_ref, wu_ref, g_ref, u_ref):
    g_ref[...] = mm(x_ref[...], wg_ref[...])
    u_ref[...] = mm(x_ref[...], wu_ref[...])


def up_kernel(meta, lg_ref, lu_ref, pg_ref, pu_ref, ad_ref, b_ref, *rest, formed, first):
    h_ref, hot_ref, pad_ref, rare_ref, g, u, delta = rest[-7:]
    ins = rest[:-7]
    s = Slots(meta, h_ref.shape[0])

    if first:
        @pl.when(pl.program_id(0) == 0)
        def _():
            for ref in (hot_ref, pad_ref, rare_ref):
                ref[...] = jnp.zeros_like(ref)
    else:
        @pl.when(pl.program_id(0) == 0)
        def _():
            for ref, was in zip((hot_ref, pad_ref, rare_ref), ins[-3:]):
                ref[...] = was[...]

    if formed:
        g[...] = ins[0][...]
        u[...] = ins[1][...]
    else:
        for rs in (slice(0, HOT), slice(HOT, g.shape[0])):
            g[rs] = mm(ins[0][rs, :], ins[1][...])
            u[rs] = mm(ins[0][rs, :], ins[2][...])
    for i, (total, low_ref, part_ref) in enumerate(((g, lg_ref, pg_ref), (u, lu_ref, pu_ref))):
        for j in range(COLD):
            delta[j] = scaled(part_ref[j], b_ref[s.owner(j), i])
        total[:HOT] += scaled(low_ref[:HOT, :], b_ref[s.hot, i]).astype(F32)
        for j in range(COLD):
            total[pl.ds(s.first(j), BLK), :] += delta[j].astype(F32)

    def visit(owner, rs, mask):
        g[rs, :] += scaled(jnp.where(mask, lg_ref[rs, :].astype(F32), 0.0).astype(BF), b_ref[owner, 0]).astype(F32)
        u[rs, :] += scaled(jnp.where(mask, lu_ref[rs, :].astype(F32), 0.0).astype(BF), b_ref[owner, 1]).astype(F32)

    s.extras(visit)
    for r in range(0, h_ref.shape[0], 256):
        rs = slice(r, r + 256)
        h_ref[rs] = (jax.nn.silu(g[rs]) * u[rs]).astype(BF)
    hot_ref[...] += mm_nt(h_ref[:HOT, :], ad_ref[s.hot])
    for j in range(COLD):
        pad_ref[j] += mm_nt(h_ref[pl.ds(s.first(j), BLK), :], ad_ref[s.owner(j)])

    def visit_d(owner, rs, mask):
        rare_ref[rs, :] += jnp.where(mask, mm_nt(h_ref[rs, :], ad_ref[owner]), 0.0)

    s.extras(visit_d)


def part_kernel(h_ref, w_ref, *rest):
    y_ref = rest[-1]
    acc = mm(h_ref[...], w_ref[...])
    y_ref[...] = acc if len(rest) == 1 else acc + rest[0][...]


def down_kernel(meta, rank_ref, loc_ref, hot_ref, pad_ref, rare_ref, xs_ref, yin_ref, b_ref, o_ref, perm, low, pad, y, dy):
    s = Slots(meta, xs_ref.shape[0])

    @pl.when(pl.program_id(0) == 0)
    def _():
        col = lax.broadcasted_iota(jnp.int32, perm.shape, 1)
        perm[...] = jnp.where(col == rank_ref[...], 1.0, 0.0).astype(BF)
        total = rare_ref
        own = (lax.broadcasted_iota(jnp.int32, total.shape, 1) // 8) == loc_ref[...]
        low[...] = jnp.where(own, total[...], 0.0).astype(BF)
        low[:HOT] = jnp.where(own[:HOT], hot_ref[...], 0.0).astype(BF)
        col = lax.broadcasted_iota(jnp.int32, (BLK, 256), 1) // 8
        for j in range(COLD):
            keep = (col == loc_ref[pl.ds(s.first(j), BLK), :]) & s.mask(j)
            pad[j] = jnp.where(keep, pad_ref[j], 0.0).astype(BF)

    for j in range(COLD):
        dy[j] = scaled(pad[j], b_ref[s.owner(j)])
    y[...] = yin_ref[...]
    y[:HOT] += scaled(low[:HOT, :], b_ref[s.hot]).astype(F32)
    for j in range(COLD):
        y[pl.ds(s.first(j), BLK), :] += dy[j].astype(F32)

    def visit(owner, rs, mask):
        y[rs, :] += scaled(jnp.where(mask, low[rs, :].astype(F32), 0.0).astype(BF), b_ref[owner]).astype(F32)

    s.extras(visit)
    done = (xs_ref[...].astype(F32) + y[...]).astype(BF)
    o_ref[...] = mm(perm[...], done).astype(BF)


def params(limit=VMEM_LIMIT):
    return pltpu.CompilerParams(vmem_limit_bytes=limit, dimension_semantics=('arbitrary',))


def const(shape):
    return pl.BlockSpec(shape, lambda i, *_: (0,) * len(shape), pipeline_mode=pl.Buffered(1))


def cols(shape, off=0):
    lead = (0,) * (len(shape) - 1)
    return pl.BlockSpec(shape, lambda i, *_: lead + (i + off,))


def row_part(rows, width, off):
    return pl.BlockSpec((pl.Element(rows), pl.Element(width)), lambda i, *_: (off, i * width))


def shape(dims, dtype):
    return jax.ShapeDtypeStruct(dims, dtype)


def cost(flops, nbytes, trans=0):
    return pl.CostEstimate(flops=int(flops), bytes_accessed=int(nbytes), transcendentals=trans)


def sort_call(meta, rank_row, loc_col, hidden, ag, au):
    rows, d = hidden.shape
    low, pad = (rows, 256), (COLD, BLK, 256)
    return pl.pallas_call(
        sort_kernel,
        grid_spec=pltpu.PrefetchScalarGridSpec(
            num_scalar_prefetch=1, grid=(d // TK,),
            in_specs=[const((1, rows)), const((rows, 1)), cols((rows, TK)), cols((8, 256, TK)), cols((8, 256, TK))],
            out_specs=[cols((rows, TK)), const(low), const(low), const(pad), const(pad)],
            scratch_shapes=[pltpu.VMEM((rows, rows), BF), pltpu.VMEM(low, F32), pltpu.VMEM(low, F32), pltpu.VMEM(pad, F32), pltpu.VMEM(pad, F32)]),
        out_shape=[shape((rows, d), BF), shape(low, BF), shape(low, BF), shape(pad, BF), shape(pad, BF)],
        compiler_params=params(58 * 2**20),
        cost_estimate=cost(2 * rows * d * (rows + 700), 4 * rows * d + 8192 * d),
        name='sort_rows',
    )(meta, rank_row, loc_col, hidden, ag, au)


def pack_call(bg, bu, off, width):
    f = width * TF
    return pl.pallas_call(
        pack_kernel,
        grid=(width,),
        in_specs=[cols((256, TF), off)] * 2,
        out_specs=cols((2, 256, TF)),
        out_shape=shape((2, 256, f), BF),
        compiler_params=params(62 * 2**20),
        cost_estimate=cost(0, 2048 * f),
        name='pack',
    )(bg, bu)


def base_call(xs, wg, wu, off, width):
    rows, d = xs.shape
    f = width * TF
    return pl.pallas_call(
        base_kernel,
        grid=(width,),
        in_specs=[WHOLE, cols((d, TF), off), cols((d, TF), off)],
        out_specs=[cols((rows, TF))] * 2,
        out_shape=[shape((rows, f), F32)] * 2,
        compiler_params=params(40 * 2**20),
        cost_estimate=cost(4 * rows * d * f, 4 * d * f + 2 * rows * d + 8 * rows * f),
        name='base',
    )(xs, wg, wu)


def up_call(meta, xs, wg, wu, lows, ad, b, acc, off, width, base=None):
    rows, d = xs.shape
    f = width * TF
    low, pad = (rows, 256), (COLD, BLK, 256)
    if base is None:
        ins, specs = [xs, wg, wu], [WHOLE, cols((d, TF), off), cols((d, TF), off)]
    else:
        ins, specs = list(base), [cols((rows, TF))] * 2
    accs = [] if acc is None else list(acc)
    aliases = {7 + len(ins) + i: 1 + i for i in range(len(accs))}
    return pl.pallas_call(
        functools.partial(up_kernel, formed=base is not None, first=acc is None),
        grid_spec=pltpu.PrefetchScalarGridSpec(
            num_scalar_prefetch=1, grid=(width,),
            in_specs=[const(low), const(low), const(pad), const(pad), cols((8, 256, TF), off), cols((8, 2, 256, TF))] + specs + [WHOLE] * len(accs),
            out_specs=[cols((rows, TF))] + [WHOLE] * 3,
            scratch_shapes=[pltpu.VMEM((rows, TF), F32), pltpu.VMEM((rows, TF), F32), pltpu.VMEM((COLD, BLK, TF), BF)]),
        out_shape=[shape((rows, f), BF), shape((HOT, 256), F32), shape(pad, F32), shape(low, F32)],
        input_output_aliases=aliases,
        compiler_params=params(UP_LIMIT),
        cost_estimate=cost(4 * rows * d * f * (0.2 if base else 1.2), (8 * rows if base else 4 * d) * f + 2 * rows * f + 12288 * f, rows * f),
        name='finish' if base else 'gate_up',
    )(meta, *lows, ad, b, *ins, *accs)


def part_call(h, w, y, off):
    rows, f = h.shape
    d = w.shape[1]
    extra = [] if y is None else [y]
    return pl.pallas_call(
        part_kernel,
        grid=(d // TD,),
        in_specs=[const(h.shape), row_part(f, TD, off * TF)] + [cols((rows, TD))] * len(extra),
        out_specs=cols((rows, TD)),
        out_shape=shape((rows, d), F32),
        input_output_aliases={2: 0} if extra else {},
        compiler_params=params(40 * 2**20),
        cost_estimate=cost(2 * rows * d * f, 2 * d * f + 2 * rows * f + 8 * rows * d),
        name='down_part',
    )(h, w, *extra)


def down_call(meta, rank_col, loc_col, acc, xs, y, b):
    rows, d = xs.shape
    low, pad = (rows, 256), (COLD, BLK, 256)
    return pl.pallas_call(
        down_kernel,
        grid_spec=pltpu.PrefetchScalarGridSpec(
            num_scalar_prefetch=1, grid=(d // TD,),
            in_specs=[const((rows, 1)), const((rows, 1)), const((HOT, 256)), const(pad), const(low), cols((rows, TD)),
                      cols((rows, TD)), cols((8, 256, TD))],
            out_specs=cols((rows, TD)),
            scratch_shapes=[pltpu.VMEM((rows, rows), BF), pltpu.VMEM(low, BF), pltpu.VMEM(pad, BF), pltpu.VMEM((rows, TD), F32), pltpu.VMEM((COLD, BLK, TD), BF)]),
        out_shape=shape((rows, d), BF),
        compiler_params=params(),
        cost_estimate=cost(2 * rows * d * (rows + 512), 2 * (2 * rows * d + 2048 * d) + 4 * rows * d),
        name='down',
    )(meta, rank_col, loc_col, *acc, xs, y, b)


def gather(own):
    return lax.all_gather(own, 'data', axis=0, tiled=False)


def solution(mesh):
    row_spec = P(('rep', 'data'), None)
    tok_spec = P(('rep', 'data'))
    full_two = P(None, None)
    full_three = P(None, None, None)
    owned = P('data', None, None)

    def device_fn(hidden, adapter_id, w_gate, w_up, w_down, a_gate, b_gate, a_up, b_up, a_down, b_down):
        rows, d = hidden.shape
        f = w_gate.shape[1]
        bg, bu, bd = b_gate.reshape(256, f), b_up.reshape(256, f), b_down.reshape(256, d)
        ag, au, ad = (jnp.swapaxes(a, 1, 2).reshape(8, 256, a.shape[1]) for a in (a_gate, a_up, a_down))

        packs, offs, off = [], [], 0
        for width in CHUNKS:
            packs.append(gather(pack_call(bg, bu, off, width)))
            offs.append(off)
            off += width
        b_all = gather(bd)

        owner = adapter_id // 32
        owners = jnp.arange(8, dtype=jnp.int32)
        token = jnp.arange(rows, dtype=jnp.int32)
        count = jnp.sum((owner[:, None] == owners[None, :]).astype(jnp.int32), axis=0)
        hot = jnp.argmax(count).astype(jnp.int32)
        key = jnp.where(owner == hot, -1, owner)
        before = (key[None, :] < key[:, None]) | ((key[None, :] == key[:, None]) & (token[None, :] < token[:, None]))
        rank = jnp.sum(before.astype(jnp.int32), axis=1)
        loc = jnp.sum(jnp.where(rank[None, :] == token[:, None], (adapter_id % 32)[None, :], 0), axis=1)
        cold = jnp.arange(COLD, dtype=jnp.int32)
        cold = cold + (cold >= hot).astype(jnp.int32)
        start = HOT + jnp.sum(jnp.where((owners[None, :] < cold[:, None]) & (owners[None, :] != hot), count[None, :], 0), axis=1)
        end = start + jnp.sum(jnp.where(owners[None, :] == cold[:, None], count[None, :], 0), axis=1)
        extra = jnp.any(end - (start // 16) * 16 > BLK).astype(jnp.int32)
        zero = jnp.zeros((1,), jnp.int32)
        meta = jnp.concatenate([jnp.stack([hot, extra]), jnp.zeros((6,), jnp.int32), cold, zero, start, zero, end, zero]).astype(jnp.int32)

        xs, *lows = sort_call(meta, rank[None, :], loc[:, None], hidden, ag, au)
        base = base_call(xs, w_gate, w_up, offs[-1], CHUNKS[-1])
        acc = y = None
        final = len(CHUNKS) - 1
        for i, (pack, first, width) in enumerate(zip(packs, offs, CHUNKS)):
            h, *acc = up_call(meta, xs, w_gate, w_up, lows, ad, pack, acc, first, width, base if i == final else None)
            y = part_call(h, w_down, y, first)
            if i < final:
                acc, y = lax.optimization_barrier((acc, y))
        return down_call(meta, rank[:, None], loc[:, None], acc, xs, y, b_all)

    return jax.shard_map(device_fn, mesh=mesh, in_specs=(row_spec, tok_spec, full_two, full_two, full_two, full_three, owned, full_three, owned, full_three, owned), out_specs=row_spec, check_vma=False)
```
